512 devices in a mesh: box: 128 (over y, z, core), nbr: 4 (over x).
Axes of the slice: x: 4, y: 8, z: 8, core: 2. Of those that a mesh axis runs over, the one named last changes fastest.
Arguments:
- self_block: float32 [1024, 256, 256], P('box', 'nbr'), as said below
- ordering: int32 [1024, 256], P('box'), may hold values from 0 to 255, each once within a row
- interp: float32 [1024, 64, 192], P('box'), may hold values from -0.12 to 0.12
- near_band: float32 [1024, 8, 2, 64, 256], P('box', 'nbr'), may hold values from -3 to 3
- pair_mask: int32 [1024, 8], P('box', 'nbr'), may hold values 0 or 1
Outputs:
- skeleton_self: float32 [1024, 64, 64], P('box')
- red_inverse: float32 [1024, 192, 192], P('box', 'nbr')
- couplings: float32 [1024, 8, 64, 128], P('box', 'nbr')
The draws below stay inside these ranges and needn't reach their ends.
Inputs may be any that keep to these rules, and one draw needn't show every extreme that they name: Each row of ordering is a permutation of the 256 unknowns of its box. Each self_block[b] has a positive diagonal.
All inputs are finite; a program needn't handle non-finite values. No bound on the sum of `pair_mask` on one device may be relied on, other than what follows from the above.
Results may differ from the reference program's by a relative error of at most 0.0003.
Values sent between devices are 32-bit elements; how exact they have to be, the bound alone decides.
No kernel may reach another device: no remote copies, remote signals or barrier semaphores. Data moves between devices by JAX's collectives and lax.ppermute only.
A program may use at most 128 MiB of HBM per device.

```python
import jax
import jax.numpy as jnp
from jax import lax

PTS = 256
SKEL = 64
RED = 192
REACH = 4
OFFS = 8
NS_ITERS = 3
BOX_DEV = 8
BOXES = 1024


def draw_self_block(key, part):
    first_key, second_key = jax.random.split(jax.random.fold_in(key, 17), 2)
    diag_vals = jax.random.uniform(first_key, (BOXES, PTS), jnp.float32, 8.0, 16.0)
    spread = 0.2 * jnp.clip(jax.random.normal(second_key, (BOXES, PTS, PTS), jnp.float32), -4.0, 4.0)
    identity = jnp.eye(PTS, dtype=jnp.float32)[None]
    return spread * (1.0 - identity) + identity * diag_vals[:, None, :]


def set_ends(values, own_key, least, top_value):
    index_at = [jax.random.randint(jax.random.fold_in(own_key, axis), (), 0, length) for axis, length in enumerate(values.shape)]
    longest = values.shape.index(max(values.shape))
    beside = index_at[:longest] + [(index_at[longest] + 1) % values.shape[longest]] + index_at[longest + 1:]
    return values.at[tuple(index_at)].set(least).at[tuple(beside)].set(top_value)


def shard_levels(own_key, extent, cuts, smallest, largest):
    factor_of = 1.0
    for axis_at, shards_of in cuts:
        heights = jax.random.uniform(jax.random.fold_in(jax.random.fold_in(own_key, 6), axis_at), (shards_of,), jnp.float32, smallest / len(cuts), largest / len(cuts))
        factor_of = factor_of * jnp.repeat(jnp.exp(heights), extent[axis_at] // shards_of).reshape((-1,) + (1,) * (len(extent) - 1 - axis_at))
    return factor_of


def gaussian(stream_key, dims, scale, reach, cuts=(), kind=jnp.bfloat16):
    entries = jax.random.normal(stream_key, dims, jnp.float32) * scale
    if len(cuts) > 0:
        entries = shard_levels(stream_key, dims, cuts, -0.22, 0.18) * entries
    return jnp.clip(entries, min=-reach, max=reach).astype(kind)


def setup_inputs(seed: int = 0) -> dict:
    key_of = jax.random.split(jax.random.key(seed), 6)
    return {
        "self_block": draw_self_block(jax.random.fold_in(key_of[5], 71), 0),
        "ordering": jax.vmap(lambda own: jax.random.permutation(own, PTS))(jax.random.split(key_of[1], BOXES)).reshape((BOXES, PTS)).astype(jnp.int32),
        "interp": gaussian(key_of[2], (BOXES, SKEL, RED), 0.02, 0.12, ((0, 128),), jnp.float32),
        "near_band": gaussian(key_of[3], (BOXES, OFFS, 2, SKEL, PTS), 0.5, 3.0, ((0, 128), (1, 4)), jnp.float32),
        "pair_mask": set_ends((jax.random.randint(key_of[4], (BOXES, OFFS), 0, 4) < 3).astype(jnp.int32), jax.random.fold_in(key_of[4], 1), 0, 1),
    }


def product(pattern, left_term, right_term):
    return jnp.einsum(pattern, left_term, right_term, precision=lax.Precision.HIGHEST)


def permuted(matrix, ordering):
    row_sorted = jnp.take_along_axis(matrix, ordering[:, :, None], axis=1)
    return jnp.take_along_axis(row_sorted, ordering[:, None, :], axis=2)


def factors(matrix, ordering, interp):
    full_block = permuted(matrix, ordering)
    skel_skel = full_block[:, :SKEL, :SKEL]
    skel_red = full_block[:, :SKEL, SKEL:]
    red_skel = full_block[:, SKEL:, :SKEL]
    red_red = full_block[:, SKEL:, SKEL:]
    skel_interp = product("bij,bjk->bik", skel_skel, interp)
    x_skel_red = skel_red - skel_interp
    x_red_skel = red_skel - product("bji,bjk->bik", interp, skel_skel)
    x_red_red = red_red - product("bji,bjk->bik", interp, skel_red) - product("bij,bjk->bik", red_skel, interp)
    x_red_red = x_red_red + product("bji,bjk->bik", interp, skel_interp)
    identity = jnp.eye(RED, dtype=jnp.float32)
    diag_vals = jnp.diagonal(red_red, axis1=1, axis2=2)
    approx = identity[None] / diag_vals[:, None, :]
    for sweep_index in range(NS_ITERS):
        approx = 2.0 * approx - product("bij,bjk->bik", approx, product("bij,bjk->bik", x_red_red, approx))
    left_factor = product("bij,bjk->bik", x_skel_red, approx)
    right_factor = product("bij,bjk->bik", approx, x_red_skel)
    own_block = skel_skel - product("bij,bjk->bik", left_factor, x_red_skel)
    return approx, left_factor, right_factor, own_block


def slot_terms(near_piece, ordering, interp, approx, left_factor, right_factor):
    row_part = jnp.take_along_axis(near_piece[:, 0], ordering[:, None, :], axis=2)
    col_part = jnp.take_along_axis(near_piece[:, 1], ordering[:, None, :], axis=2)
    near_red = row_part[:, :, SKEL:] - product("bij,bjk->bik", row_part[:, :, :SKEL], interp)
    red_near_t = col_part[:, :, SKEL:] - product("bij,bjk->bik", col_part[:, :, :SKEL], interp)
    new_forward = jnp.swapaxes(col_part[:, :, :SKEL], 1, 2) - product("bij,bkj->bik", left_factor, red_near_t)
    new_backward = jnp.swapaxes(row_part[:, :, :SKEL], 1, 2) - product("bji,bkj->bik", right_factor, near_red)
    coupled = jnp.concatenate([new_forward, new_backward], axis=2)
    update = product("bij,bkj->bik", product("bij,bjk->bik", near_red, approx), red_near_t)
    return coupled, update


def reference(self_block, ordering, interp, near_band, pair_mask):
    offsets = [slot_index - REACH if slot_index < REACH else slot_index - REACH + 1 for slot_index in range(OFFS)]
    box_total = self_block.shape[0]
    groups = box_total // BOX_DEV

    def one_group(group_index):
        first_box = group_index * BOX_DEV
        box_ids = first_box + jnp.arange(BOX_DEV, dtype=jnp.int32)
        matrix = lax.dynamic_slice_in_dim(self_block, first_box, BOX_DEV, 0)
        order_part = lax.dynamic_slice_in_dim(ordering, first_box, BOX_DEV, 0)
        interp_part = lax.dynamic_slice_in_dim(interp, first_box, BOX_DEV, 0)
        approx, left_factor, right_factor, own_block = factors(matrix, order_part, interp_part)
        couples = []
        updates = []
        for slot_index in range(OFFS):
            source = ((box_ids - offsets[slot_index]) % box_total).astype(jnp.int32)
            weight = pair_mask[source, slot_index].astype(jnp.float32)
            near_piece = near_band[source, slot_index] * weight[:, None, None, None]
            coupled, update = slot_terms(near_piece, order_part, interp_part, approx, left_factor, right_factor)
            couples.append(coupled)
            updates.append(update)
        return own_block, approx, jnp.stack(couples, 1), jnp.stack(updates, 1)

    own_all, approx_all, couple_all, update_all = lax.map(one_group, jnp.arange(groups, dtype=jnp.int32))
    own_all = own_all.reshape(box_total, SKEL, SKEL)
    update_all = update_all.reshape(box_total, OFFS, SKEL, SKEL)
    summed = jnp.zeros_like(own_all)
    for slot_index in range(OFFS):
        summed = summed + jnp.roll(update_all[:, slot_index], -offsets[slot_index], axis=0)
    skeleton_self = own_all - summed
    red_inverse = approx_all.reshape(box_total, RED, RED)
    couplings = couple_all.reshape(box_total, OFFS, SKEL, 2 * SKEL)
    return skeleton_self, red_inverse, couplings
```

```python
import jax
import jax.numpy as jnp
from jax import lax
from jax.experimental import pallas as pl
from jax.experimental.pallas import tpu as pltpu
from jax.sharding import PartitionSpec as P

SKEL = 64
RED = 192
PTS = 256
REACH = 4
HALF = 4
PAIR = 128
ROWS = 48
BF = jnp.bfloat16
F32 = jnp.float32
LIMIT = 28 * 1024 * 1024


def split(x):
    high = x.astype(BF)
    return high, (x - high.astype(F32)).astype(BF)


def dot(a, b):
    return jnp.dot(a, b, preferred_element_type=F32)


def dot3(a, b):
    return dot(a[0], b[0]) + dot(a[1], b[0]) + dot(a[0], b[1])


def eye(rows, columns):
    i = lax.broadcasted_iota(jnp.int32, (rows, columns), 0)
    j = lax.broadcasted_iota(jnp.int32, (rows, columns), 1)
    return (i == j).astype(F32)


def slot_offset(place, slot):
    j = place * 2 + slot
    return jnp.where(j < REACH, j - REACH, j - REACH + 1)


def half_of(place, chunk):
    return jnp.where(place < 2, 1 - chunk, chunk)


def choose(boxes, order_ref, interp, mixer, z_ref, zt_ref):
    unknown = lax.broadcasted_iota(jnp.int32, (PTS, PTS), 0)
    upper = eye(RED, PTS).astype(BF)
    nothing = jnp.zeros((RED, PTS), BF)
    for k, box in enumerate(boxes):
        low = jnp.concatenate([-interp[k], eye(SKEL, SKEL)], axis=1)
        mixer[k, 0, :RED], mixer[k, 1, :RED] = upper, nothing
        mixer[k, 0, RED:], mixer[k, 1, RED:] = split(low)
    for k, box in enumerate(boxes):
        order = pltpu.roll(order_ref[pl.ds(box, 1), :], RED, 1)
        chooser = (unknown == order).astype(F32).astype(BF)
        for level in range(2):
            z = dot(chooser, mixer[k, level])
            z_ref[k, level] = z.astype(BF)
            zt_ref[k, level] = z.T.astype(BF)


def source_of(box, place, slot):
    source = box - slot_offset(place, slot)
    inside = jnp.logical_and(source >= 0, source < 2 * HALF)
    return source, inside, jnp.clip(source, 0, 2 * HALF - 1)


def fetch(boxes, place, near_ref, halo_ref, rows_ref, sem):
    waits = []
    for k, box in enumerate(boxes):
        for slot in range(2):
            source, inside, local = source_of(box, place, slot)
            to = rows_ref.at[k, slot]
            flag = sem.at[2 * k + slot]
            near = pltpu.make_async_copy(near_ref.at[local, slot], to, flag)
            waits.append(near)
            if halo_ref is None:
                near.start()
            else:
                remote = jnp.where(source >= 2 * HALF, source - 2 * HALF, source + HALF)
                remote = jnp.clip(remote, 0, HALF - 1)
                far = pltpu.make_async_copy(halo_ref.at[remote, slot], to, flag)
                pl.when(inside)(near.start)
                pl.when(jnp.logical_not(inside))(far.start)
    return waits


def meet(boxes, place, mask_ref, rows_ref, z_ref):
    g, nt = [], []
    for k, box in enumerate(boxes):
        rows = []
        for slot in range(2):
            _, inside, local = source_of(box, place, slot)
            weight = jnp.where(inside, mask_ref[local, slot], 1).astype(F32)
            rows.append(rows_ref[k, slot] * weight)
        stacked = jnp.concatenate([rows[0][0], rows[1][0], rows[0][1], rows[1][1]], axis=0)
        done = dot3(split(stacked), (z_ref[k, 0], z_ref[k, 1]))
        g.append(done[:PAIR])
        nt.append(done[PAIR:].T)
    return g, nt


def factor(place, blocks_ref, z_ref, zt_ref, even, odd, tail, inverse_ref):
    each = range(HALF)
    diagonal = eye(PTS, PTS)
    red_diag = diagonal[:RED]
    column = lax.broadcasted_iota(jnp.int32, (1, PTS), 1)
    moved, diag_row, block, inv = [], [], [], []
    for k in each:
        full = blocks_ref[:, k].reshape(PTS, PTS)
        diag_row.append(jnp.sum(full * diagonal, axis=0, keepdims=True))
        moved.append(split(dot3(split(full), (z_ref[k, 0], z_ref[k, 1]))))
    for k in each:
        block.append(dot3((zt_ref[k, 0], zt_ref[k, 1]), moved[k]))
    for k in each:
        chosen = zt_ref[k, 0].astype(F32)
        order_col = jnp.sum(jnp.where(chosen == 1.0, diag_row[k], 0.0), axis=1, keepdims=True)
        scale = jnp.sum(diagonal * order_col, axis=0, keepdims=True)
        inv.append(jnp.where(column < RED, 1.0 / jnp.where(column < RED, scale, 1.0), 0.0))
    nothing = jnp.zeros((SKEL, PTS), BF)
    e1, e1s, e2, s4 = [], [], [], []
    for k in each:
        for ref in (even, odd):
            ref[k, 0, RED:], ref[k, 1, RED:] = nothing, nothing
        e1.append(jnp.where(column < RED, red_diag - block[k][:RED] * inv[k], 0.0))
        e1s.append(split(e1[k]))
        even[k, 0, :RED], even[k, 1, :RED] = e1s[k]
    for k in each:
        e2.append(dot3(e1s[k], (even[k, 0], even[k, 1])))
        odd[k, 0, :RED], odd[k, 1, :RED] = split(e2[k])
    for k in each:
        e2s = (odd[k, 0, :RED], odd[k, 1, :RED])
        e4 = dot3(e2s, (odd[k, 0], odd[k, 1]))
        s4.append(red_diag + e1[k] + e2[k] + dot3(e1s[k], (odd[k, 0], odd[k, 1])))
        even[k, 0, :RED], even[k, 1, :RED] = split(e4)
    for k in each:
        s8 = s4[k] + dot3(split(s4[k]), (even[k, 0], even[k, 1]))
        odd[k, 0, :RED], odd[k, 1, :RED] = split(s8)
        tail[k] = s8
    i = lax.broadcasted_iota(jnp.int32, (ROWS, PTS), 0) + place * ROWS
    j = lax.broadcasted_iota(jnp.int32, (ROWS, PTS), 1)
    start = pl.multiple_of(place * ROWS, 8)
    for k in each:
        inv_col = jnp.sum(jnp.where(i == j, inv[k], 0.0), axis=1, keepdims=True)
        inverse_ref[k] = (tail[k, pl.ds(start, ROWS), :] * inv_col)[:, :RED]
    skel = [block[k][RED:] for k in each]
    side = [block[k][:, PAIR:] for k in each]
    return inv, skel, side


def finish(boxes, place, inv, skel, side, g, nt, s_ref, couple_ref, own_ref, extended):
    each = range(HALF)
    lane = lax.broadcasted_iota(jnp.int32, (SKEL, PAIR), 1)
    left = lane < SKEL
    carried, last = [], []
    for k in each:
        mine = jnp.concatenate([skel[k], g[k]], axis=0) * inv[k]
        carried.append(dot3(split(mine), (s_ref[k, 0], s_ref[k, 1])))
    for k in each:
        right = split(jnp.concatenate([nt[k], side[k]], axis=1))
        last.append(dot3(split(carried[k]), right))
    for k in each:
        end = last[k]
        own_ref[k] = (skel[k][:, PAIR:] - end[:SKEL, PAIR:])[:, SKEL:]
        forward = nt[k][RED:] - end[:SKEL, :PAIR]
        backward = (g[k][:, PAIR:] - end[SKEL:, PAIR:]).T[SKEL:]
        couple_ref[k, 0] = jnp.where(left, forward, pltpu.roll(backward, SKEL, 1))
        couple_ref[k, 1] = jnp.where(left, pltpu.roll(forward, SKEL, 1), backward)
    for k, box in enumerate(boxes):
        first = box - slot_offset(place, 0) + REACH
        second = box - slot_offset(place, 1) + REACH
        extended[first] += jnp.where(left, last[k][SKEL:PAIR, :PAIR], 0.0)
        extended[second] += jnp.where(left, 0.0, last[k][PAIR:, :PAIR])
    return left


def doubled(x):
    return x + pltpu.roll(x, SKEL, 1)


def packed(extended, left):
    return [
        jnp.where(left, doubled(extended[REACH + k]), doubled(extended[REACH + HALF + k]))
        for k in range(HALF)
    ]


def boxes_of(place, chunk):
    base = half_of(place, chunk) * HALF
    return [base + k for k in range(HALF)]


def started(copies):
    for copy in copies:
        copy.start()
    return copies


def ended(copies):
    for copy in copies:
        copy.wait()


def half_rows(ref, place, chunk):
    return ref.at[pl.ds(half_of(place, chunk) * HALF, HALF)]


def factor_kernel(
    place_ref, order_ref, interp_ref, first_ref,
    inverse_ref, z_ref, s_ref, inv_ref, skel_ref, side_ref,
    blocks_ref, interp, zt_ref, even, tail, sem,
):
    place = place_ref[0]
    needs = started([
        pltpu.make_async_copy(half_rows(interp_ref, place, 0), interp, sem.at[0]),
        pltpu.make_async_copy(first_ref, blocks_ref, sem.at[1]),
    ])
    ended(needs[:1])
    choose(boxes_of(place, 0), order_ref, interp, even, z_ref, zt_ref)
    ended(needs[1:])
    inv, skel, side = factor(place, blocks_ref, z_ref, zt_ref, even, s_ref, tail, inverse_ref)
    for k in range(HALF):
        inv_ref[k] = jnp.broadcast_to(inv[k], (8, PTS))
        skel_ref[k], side_ref[k] = skel[k], side[k]


def edge_kernel(
    place_ref, mask_ref, near_ref, halo_ref, z_ref, s_ref, inv_ref, skel_ref, side_ref,
    couple_ref, own_ref, kept_ref, leaving_ref, rows_ref, extended, sem,
):
    place = place_ref[0]
    boxes = boxes_of(place, 0)
    waits = fetch(boxes, place, near_ref, halo_ref, rows_ref, sem)
    extended[...] = jnp.zeros_like(extended)
    ended(waits)
    g, nt = meet(boxes, place, mask_ref, rows_ref, z_ref)
    inv = [inv_ref[k, :1] for k in range(HALF)]
    skel = [skel_ref[k] for k in range(HALF)]
    side = [side_ref[k] for k in range(HALF)]
    left = finish(boxes, place, inv, skel, side, g, nt, s_ref, couple_ref, own_ref, extended)
    for k, value in enumerate(packed(extended, left)):
        kept_ref[k] = value
    beyond = jnp.where(place < 2, REACH + 2 * HALF, 0)
    for k in range(HALF):
        leaving_ref[k] = doubled(extended[beyond + k])


def inner_kernel(
    place_ref, mask_ref, order_ref, interp_ref, near_ref, block_ref, came_1, came_2, came_3,
    kept_in, inverse_in, couple_in, own_in,
    inverse_ref, couple_ref, own_ref, total_ref,
    blocks_ref, interp, rows_ref, z_ref, zt_ref, even, odd, tail, extended, sem,
):
    place = place_ref[0]
    boxes = boxes_of(place, 1)
    text = started([pltpu.make_async_copy(half_rows(interp_ref, place, 1), interp, sem.at[8])])
    parts = started([
        pltpu.make_async_copy(source, blocks_ref.at[lax.rem(place + 4 - k, 4)], sem.at[9 + k])
        for k, source in enumerate([half_rows(block_ref, place, 1), came_1, came_2, came_3])
    ])
    waits = fetch(boxes, place, near_ref, None, rows_ref, sem)
    extended[...] = jnp.zeros_like(extended)
    ended(text)
    choose(boxes, order_ref, interp, even, z_ref, zt_ref)
    ended(parts)
    inv, skel, side = factor(place, blocks_ref, z_ref, zt_ref, even, odd, tail, inverse_ref)
    ended(waits)
    g, nt = meet(boxes, place, mask_ref, rows_ref, z_ref)
    left = finish(boxes, place, inv, skel, side, g, nt, odd, couple_ref, own_ref, extended)
    for k, value in enumerate(packed(extended, left)):
        total_ref[k] = value + kept_in[k]


def call(kernel, place, args, outs, scratch, aliases=None):
    def spec(x):
        if isinstance(x, pl.BlockSpec):
            return x
        shape = x.shape
        return pl.BlockSpec(shape, lambda i, p: (0,) * len(shape))

    return pl.pallas_call(
        kernel,
        grid_spec=pltpu.PrefetchScalarGridSpec(
            num_scalar_prefetch=1,
            grid=(1,),
            in_specs=[spec(s) for _, s in args],
            out_specs=[spec(s) for _, s in outs],
            scratch_shapes=scratch,
        ),
        out_shape=[o for o, _ in outs],
        input_output_aliases=aliases or {},
        compiler_params=pltpu.CompilerParams(vmem_limit_bytes=LIMIT),
    )(place, *[a for a, _ in args])


def whole(x):
    return (x, x)


def part(x, index):
    shape = (HALF, *x.shape[1:])
    if callable(index):
        return (x, pl.BlockSpec(shape, lambda i, p: (index(p[0]),) + (0,) * (len(shape) - 1)))
    return (x, pl.BlockSpec(shape, lambda i, p: (index,) + (0,) * (len(shape) - 1)))


def smem(x):
    return (x, pl.BlockSpec(memory_space=pltpu.SMEM))


def untouched(x):
    return (x, pl.BlockSpec(memory_space=pl.ANY))


def shape(*s, dtype=F32):
    return jax.ShapeDtypeStruct(s, dtype)


def toward(box_count, nbr_count, receive):
    pairs = []
    for box in range(box_count):
        for place in range(nbr_count):
            step = 1 if (place < nbr_count // 2) == receive else -1
            other = (box + step) % box_count
            pairs.append((other * nbr_count + place, box * nbr_count + place))
    return pairs


def exchanged(x):
    return lax.all_to_all(x, "nbr", 0, 0, tiled=True).reshape(4, -1, *x.shape[1:])


def copies_kernel(place_ref, block_ref, first_ref, *rest):
    later, sem = rest[:3], rest[3]
    place = place_ref[0]
    copies = []
    for target in range(4):
        half = HALF * (1 if target < 2 else 0)
        copies.append((half, first_ref.at[pl.ds(target * HALF, HALF)]))
    for k in range(3):
        target = lax.rem(place + k + 1, 4)
        copies.append((HALF * half_of(target, 1), later[k]))
    copies = [
        pltpu.make_async_copy(block_ref.at[pl.ds(half, HALF)], out, sem.at[k])
        for k, (half, out) in enumerate(copies)
    ]
    for copy in copies:
        copy.start()
    for copy in copies:
        copy.wait()


def copies(place, self_block):
    anywhere = pl.BlockSpec(memory_space=pl.ANY)
    rest = self_block.shape[1:]
    return pl.pallas_call(
        copies_kernel,
        in_specs=[
            pl.BlockSpec(memory_space=pltpu.SMEM), pl.BlockSpec(memory_space=pltpu.VMEM),
        ],
        out_specs=[anywhere] * 4,
        out_shape=[shape(4 * HALF, *rest)] + [shape(HALF, *rest)] * 3,
        scratch_shapes=[pltpu.SemaphoreType.DMA((7,))],
        name="copies",
    )(place, self_block)


def whole_body(self_block, ordering, interp, near_band, pair_mask):
    boxes = ordering.shape[0]
    box_axis, nbr_axis = lax.axis_size("box"), lax.axis_size("nbr")
    place = lax.axis_index("nbr")
    low_side = place < nbr_axis // 2
    where = place.reshape(1)
    first, *later = copies(where, self_block)
    blocks_0 = exchanged(first)
    edge_start = jnp.where(low_side, 0, boxes - REACH)
    edge = lax.dynamic_slice_in_dim(near_band, edge_start, REACH, 0)
    edge_mask = jnp.where(low_side, pair_mask[:REACH], pair_mask[boxes - REACH :]).astype(F32)
    halo = lax.ppermute(
        edge * edge_mask[:, :, None, None, None],
        ("box", "nbr"),
        toward(box_axis, nbr_axis, True),
    )
    blocks_1 = []
    for k in range(3):
        turn = [(i, (i + k + 1) % nbr_axis) for i in range(nbr_axis)]
        blocks_1.append(lax.ppermute(later[k], "nbr", turn))
    wide = pltpu.VMEM((HALF, 2, PTS, PTS), BF)
    tail = pltpu.VMEM((HALF, RED, PTS), F32)
    extended = pltpu.VMEM((16, SKEL, PAIR), F32)
    all_blocks = pltpu.VMEM((4, HALF, SKEL, PTS), F32)
    all_rows = pltpu.VMEM((HALF, 2, 2, SKEL, PTS), F32)
    some_interp = pltpu.VMEM((HALF, SKEL, RED), F32)
    kept_shape = shape(HALF, SKEL, PAIR)
    pair_shape = shape(HALF, 2, PTS, PTS, dtype=BF)
    inverse_shape = shape(boxes, ROWS, RED)
    couple_shape, own_shape = shape(boxes, 2, SKEL, PAIR), shape(boxes, SKEL, SKEL)

    def halves(x, chunk):
        return part(x, lambda p: half_of(p, chunk))

    inverse, z, s, inv, skel, side = call(
        factor_kernel, where,
        [whole(ordering), untouched(interp), untouched(blocks_0)],
        [
            halves(inverse_shape, 0), whole(pair_shape), whole(pair_shape),
            whole(shape(HALF, 8, PTS)), whole(shape(HALF, SKEL, PTS)),
            whole(shape(HALF, PTS, PAIR)),
        ],
        [all_blocks, some_interp, wide, wide, tail, pltpu.SemaphoreType.DMA((2,))],
    )
    couple, own, kept, leaving = call(
        edge_kernel, where,
        [
            smem(pair_mask), untouched(near_band), untouched(halo), whole(z), whole(s), whole(inv),
            whole(skel), whole(side),
        ],
        [
            halves(couple_shape, 0), halves(own_shape, 0), whole(kept_shape), whole(kept_shape),
        ],
        [all_rows, extended, pltpu.SemaphoreType.DMA((8,))],
    )
    came = lax.ppermute(leaving, ("box", "nbr"), toward(box_axis, nbr_axis, False))
    red_inverse, couplings, own, total = call(
        inner_kernel, where,
        [
            smem(pair_mask), whole(ordering), untouched(interp), untouched(near_band),
            untouched(self_block), *[untouched(b) for b in blocks_1], whole(kept),
            untouched(inverse), untouched(couple), untouched(own),
        ],
        [
            halves(inverse_shape, 1), halves(couple_shape, 1), halves(own_shape, 1),
            whole(kept_shape),
        ],
        [
            all_blocks, some_interp, all_rows, wide, wide, wide, wide, tail, extended,
            pltpu.SemaphoreType.DMA((13,)),
        ],
        {10: 0, 11: 1, 12: 2},
    )
    lane_left = lax.broadcasted_iota(jnp.int32, (1, 1, PAIR), 2) < SKEL
    total = total + jnp.where(lane_left == low_side, came, 0.0)
    flat = total.reshape(HALF * SKEL, PAIR)
    gathered = exchanged(jnp.concatenate([flat] * 4)).sum(axis=0).reshape(HALF, SKEL, PAIR)
    update = jnp.concatenate([gathered[:, :, :SKEL], gathered[:, :, SKEL:]], axis=0)
    return own - update, red_inverse, couplings


def solution(mesh):
    placed = (
        P("box", "nbr", None),
        P("box", None),
        P("box", None, None),
        P("box", "nbr", None, None, None),
        P("box", "nbr"),
    )
    return jax.shard_map(
        whole_body,
        mesh=mesh,
        in_specs=placed,
        out_specs=(P("box", None, None), P("box", "nbr", None), P("box", "nbr", None, None)),
        check_vma=False,
    )
```

```python
import jax
import jax.numpy as jnp
from jax import lax
from jax.experimental import pallas as pl
from jax.experimental.pallas import tpu as pltpu
from jax.sharding import PartitionSpec as P

SKEL = 64
RED = 192
PTS = 256
REACH = 4
HALF = 4
PAIR = 128
ROWS = 48
BF = jnp.bfloat16
F32 = jnp.float32
LIMIT = 28 * 1024 * 1024


def split(x):
    high = x.astype(BF)
    return high, (x - high.astype(F32)).astype(BF)


def dot(a, b):
    return jnp.dot(a, b, preferred_element_type=F32)


def dot3(a, b):
    return dot(a[0], b[0]) + dot(a[1], b[0]) + dot(a[0], b[1])


def eye(rows, columns):
    i = lax.broadcasted_iota(jnp.int32, (rows, columns), 0)
    j = lax.broadcasted_iota(jnp.int32, (rows, columns), 1)
    return (i == j).astype(F32)


def slot_offset(place, slot):
    j = place * 2 + slot
    return jnp.where(j < REACH, j - REACH, j - REACH + 1)


def half_of(place, chunk):
    return jnp.where(place < 2, 1 - chunk, chunk)


def choose(boxes, order_ref, interp, mixer, z_ref, zt_ref):
    unknown = lax.broadcasted_iota(jnp.int32, (PTS, PTS), 0)
    upper = eye(RED, PTS).astype(BF)
    nothing = jnp.zeros((RED, PTS), BF)
    for k, box in enumerate(boxes):
        low = jnp.concatenate([-interp[k], eye(SKEL, SKEL)], axis=1)
        mixer[k, 0, :RED], mixer[k, 1, :RED] = upper, nothing
        mixer[k, 0, RED:], mixer[k, 1, RED:] = split(low)
    for k, box in enumerate(boxes):
        order = pltpu.roll(order_ref[pl.ds(box, 1), :], RED, 1)
        chooser = (unknown == order).astype(F32).astype(BF)
        for level in range(2):
            z = dot(chooser, mixer[k, level])
            z_ref[k, level] = z.astype(BF)
            zt_ref[k, level] = z.T.astype(BF)


def meet(boxes, place, mask_ref, near_ref, halo_ref, z_ref):
    g, nt = [], []
    for k, box in enumerate(boxes):
        rows = []
        for slot in range(2):
            source = box - slot_offset(place, slot)
            inside = jnp.logical_and(source >= 0, source < 2 * HALF)
            local = jnp.clip(source, 0, 2 * HALF - 1)
            weight = jnp.where(inside, mask_ref[local, slot], 0).astype(F32)
            row = near_ref[local, slot] * weight
            if halo_ref is not None:
                remote = jnp.where(source >= 2 * HALF, source - 2 * HALF, source + HALF)
                remote = jnp.clip(remote, 0, HALF - 1)
                row = row + halo_ref[remote, slot] * jnp.where(inside, 0, 1).astype(F32)
            rows.append(row)
        stacked = jnp.concatenate([rows[0][0], rows[1][0], rows[0][1], rows[1][1]], axis=0)
        done = dot3(split(stacked), (z_ref[k, 0], z_ref[k, 1]))
        g.append(done[:PAIR])
        nt.append(done[PAIR:].T)
    return g, nt


def factor(place, blocks_ref, z_ref, zt_ref, even, odd, tail, inverse_ref):
    each = range(HALF)
    diagonal = eye(PTS, PTS)
    red_diag = diagonal[:RED]
    column = lax.broadcasted_iota(jnp.int32, (1, PTS), 1)
    moved, diag_row, block, inv = [], [], [], []
    for k in each:
        full = blocks_ref[:, k].reshape(PTS, PTS)
        diag_row.append(jnp.sum(full * diagonal, axis=0, keepdims=True))
        moved.append(split(dot3(split(full), (z_ref[k, 0], z_ref[k, 1]))))
    for k in each:
        block.append(dot3((zt_ref[k, 0], zt_ref[k, 1]), moved[k]))
    for k in each:
        chosen = zt_ref[k, 0].astype(F32)
        order_col = jnp.sum(jnp.where(chosen == 1.0, diag_row[k], 0.0), axis=1, keepdims=True)
        scale = jnp.sum(diagonal * order_col, axis=0, keepdims=True)
        inv.append(jnp.where(column < RED, 1.0 / jnp.where(column < RED, scale, 1.0), 0.0))
    nothing = jnp.zeros((SKEL, PTS), BF)
    e1, e1s, e2, s4 = [], [], [], []
    for k in each:
        for ref in (even, odd):
            ref[k, 0, RED:], ref[k, 1, RED:] = nothing, nothing
        e1.append(jnp.where(column < RED, red_diag - block[k][:RED] * inv[k], 0.0))
        e1s.append(split(e1[k]))
        even[k, 0, :RED], even[k, 1, :RED] = e1s[k]
    for k in each:
        e2.append(dot3(e1s[k], (even[k, 0], even[k, 1])))
        odd[k, 0, :RED], odd[k, 1, :RED] = split(e2[k])
    for k in each:
        e2s = (odd[k, 0, :RED], odd[k, 1, :RED])
        e4 = dot3(e2s, (odd[k, 0], odd[k, 1]))
        s4.append(red_diag + e1[k] + e2[k] + dot3(e1s[k], (odd[k, 0], odd[k, 1])))
        even[k, 0, :RED], even[k, 1, :RED] = split(e4)
    for k in each:
        s8 = s4[k] + dot3(split(s4[k]), (even[k, 0], even[k, 1]))
        odd[k, 0, :RED], odd[k, 1, :RED] = split(s8)
        tail[k] = s8
    i = lax.broadcasted_iota(jnp.int32, (ROWS, PTS), 0) + place * ROWS
    j = lax.broadcasted_iota(jnp.int32, (ROWS, PTS), 1)
    start = pl.multiple_of(place * ROWS, 8)
    for k in each:
        inv_col = jnp.sum(jnp.where(i == j, inv[k], 0.0), axis=1, keepdims=True)
        inverse_ref[k] = (tail[k, pl.ds(start, ROWS), :] * inv_col)[:, :RED]
    skel = [block[k][RED:] for k in each]
    side = [block[k][:, PAIR:] for k in each]
    return inv, skel, side


def finish(boxes, place, inv, skel, side, g, nt, s_ref, couple_ref, own_ref, extended):
    each = range(HALF)
    lane = lax.broadcasted_iota(jnp.int32, (SKEL, PAIR), 1)
    left = lane < SKEL
    carried, last = [], []
    for k in each:
        mine = jnp.concatenate([skel[k], g[k]], axis=0) * inv[k]
        carried.append(dot3(split(mine), (s_ref[k, 0], s_ref[k, 1])))
    for k in each:
        right = split(jnp.concatenate([nt[k], side[k]], axis=1))
        last.append(dot3(split(carried[k]), right))
    for k in each:
        end = last[k]
        own_ref[k] = (skel[k][:, PAIR:] - end[:SKEL, PAIR:])[:, SKEL:]
        forward = nt[k][RED:] - end[:SKEL, :PAIR]
        backward = (g[k][:, PAIR:] - end[SKEL:, PAIR:]).T[SKEL:]
        couple_ref[k, 0] = jnp.where(left, forward, pltpu.roll(backward, SKEL, 1))
        couple_ref[k, 1] = jnp.where(left, pltpu.roll(forward, SKEL, 1), backward)
    for k, box in enumerate(boxes):
        first = box - slot_offset(place, 0) + REACH
        second = box - slot_offset(place, 1) + REACH
        extended[first] += jnp.where(left, last[k][SKEL:PAIR, :PAIR], 0.0)
        extended[second] += jnp.where(left, 0.0, last[k][PAIR:, :PAIR])
    return left


def doubled(x):
    return x + pltpu.roll(x, SKEL, 1)


def packed(extended, left):
    return [
        jnp.where(left, doubled(extended[REACH + k]), doubled(extended[REACH + HALF + k]))
        for k in range(HALF)
    ]


def boxes_of(place, chunk):
    base = half_of(place, chunk) * HALF
    return [base + k for k in range(HALF)]


def started(copies):
    for copy in copies:
        copy.start()
    return copies


def ended(copies):
    for copy in copies:
        copy.wait()


def half_rows(ref, place, chunk):
    return ref.at[pl.ds(half_of(place, chunk) * HALF, HALF)]


def factor_kernel(
    place_ref, order_ref, interp_ref, first_ref,
    inverse_ref, z_ref, s_ref, inv_ref, skel_ref, side_ref,
    blocks_ref, interp, zt_ref, even, tail, sem,
):
    place = place_ref[0]
    needs = started([
        pltpu.make_async_copy(half_rows(interp_ref, place, 0), interp, sem.at[0]),
        pltpu.make_async_copy(first_ref, blocks_ref, sem.at[1]),
    ])
    ended(needs[:1])
    choose(boxes_of(place, 0), order_ref, interp, even, z_ref, zt_ref)
    ended(needs[1:])
    inv, skel, side = factor(place, blocks_ref, z_ref, zt_ref, even, s_ref, tail, inverse_ref)
    for k in range(HALF):
        inv_ref[k] = jnp.broadcast_to(inv[k], (8, PTS))
        skel_ref[k], side_ref[k] = skel[k], side[k]


def edge_kernel(
    place_ref, mask_ref, near_ref, halo_ref, z_ref, s_ref, inv_ref, skel_ref, side_ref,
    couple_ref, own_ref, kept_ref, leaving_ref, extended,
):
    place = place_ref[0]
    boxes = boxes_of(place, 0)
    extended[...] = jnp.zeros_like(extended)
    g, nt = meet(boxes, place, mask_ref, near_ref, halo_ref, z_ref)
    inv = [inv_ref[k, :1] for k in range(HALF)]
    skel = [skel_ref[k] for k in range(HALF)]
    side = [side_ref[k] for k in range(HALF)]
    left = finish(boxes, place, inv, skel, side, g, nt, s_ref, couple_ref, own_ref, extended)
    for k, value in enumerate(packed(extended, left)):
        kept_ref[k] = value
    beyond = jnp.where(place < 2, REACH + 2 * HALF, 0)
    for k in range(HALF):
        leaving_ref[k] = doubled(extended[beyond + k])


def inner_kernel(
    place_ref, mask_ref, order_ref, interp_ref, near_ref, block_ref, came_1, came_2, came_3,
    kept_in, inverse_in, couple_in, own_in,
    inverse_ref, couple_ref, own_ref, total_ref,
    blocks_ref, interp, z_ref, zt_ref, even, odd, tail, extended, sem,
):
    place = place_ref[0]
    boxes = boxes_of(place, 1)
    text = started([pltpu.make_async_copy(half_rows(interp_ref, place, 1), interp, sem.at[4])])
    parts = started([
        pltpu.make_async_copy(source, blocks_ref.at[lax.rem(place + 4 - k, 4)], sem.at[k])
        for k, source in enumerate([half_rows(block_ref, place, 1), came_1, came_2, came_3])
    ])
    extended[...] = jnp.zeros_like(extended)
    ended(text)
    choose(boxes, order_ref, interp, even, z_ref, zt_ref)
    ended(parts)
    inv, skel, side = factor(place, blocks_ref, z_ref, zt_ref, even, odd, tail, inverse_ref)
    g, nt = meet(boxes, place, mask_ref, near_ref, None, z_ref)
    left = finish(boxes, place, inv, skel, side, g, nt, odd, couple_ref, own_ref, extended)
    for k, value in enumerate(packed(extended, left)):
        total_ref[k] = value + kept_in[k]


def call(kernel, place, args, outs, scratch, aliases=None):
    def spec(x):
        if isinstance(x, pl.BlockSpec):
            return x
        shape = x.shape
        return pl.BlockSpec(shape, lambda i, p: (0,) * len(shape))

    return pl.pallas_call(
        kernel,
        grid_spec=pltpu.PrefetchScalarGridSpec(
            num_scalar_prefetch=1,
            grid=(1,),
            in_specs=[spec(s) for _, s in args],
            out_specs=[spec(s) for _, s in outs],
            scratch_shapes=scratch,
        ),
        out_shape=[o for o, _ in outs],
        input_output_aliases=aliases or {},
        compiler_params=pltpu.CompilerParams(vmem_limit_bytes=LIMIT),
    )(place, *[a for a, _ in args])


def whole(x):
    return (x, x)


def part(x, index):
    shape = (HALF, *x.shape[1:])
    if callable(index):
        return (x, pl.BlockSpec(shape, lambda i, p: (index(p[0]),) + (0,) * (len(shape) - 1)))
    return (x, pl.BlockSpec(shape, lambda i, p: (index,) + (0,) * (len(shape) - 1)))


def smem(x):
    return (x, pl.BlockSpec(memory_space=pltpu.SMEM))


def untouched(x):
    return (x, pl.BlockSpec(memory_space=pl.ANY))


def shape(*s, dtype=F32):
    return jax.ShapeDtypeStruct(s, dtype)


def toward(box_count, nbr_count, receive):
    pairs = []
    for box in range(box_count):
        for place in range(nbr_count):
            step = 1 if (place < nbr_count // 2) == receive else -1
            other = (box + step) % box_count
            pairs.append((other * nbr_count + place, box * nbr_count + place))
    return pairs


def exchanged(x):
    return lax.all_to_all(x, "nbr", 0, 0, tiled=True).reshape(4, -1, *x.shape[1:])


def copies_kernel(place_ref, block_ref, first_ref, *rest):
    later, sem = rest[:3], rest[3]
    place = place_ref[0]
    copies = []
    for target in range(4):
        half = HALF * (1 if target < 2 else 0)
        copies.append((half, first_ref.at[pl.ds(target * HALF, HALF)]))
    for k in range(3):
        target = lax.rem(place + k + 1, 4)
        copies.append((HALF * half_of(target, 1), later[k]))
    copies = [
        pltpu.make_async_copy(block_ref.at[pl.ds(half, HALF)], out, sem.at[k])
        for k, (half, out) in enumerate(copies)
    ]
    for copy in copies:
        copy.start()
    for copy in copies:
        copy.wait()


def copies(place, self_block):
    anywhere = pl.BlockSpec(memory_space=pl.ANY)
    rest = self_block.shape[1:]
    return pl.pallas_call(
        copies_kernel,
        in_specs=[
            pl.BlockSpec(memory_space=pltpu.SMEM), pl.BlockSpec(memory_space=pltpu.VMEM),
        ],
        out_specs=[anywhere] * 4,
        out_shape=[shape(4 * HALF, *rest)] + [shape(HALF, *rest)] * 3,
        scratch_shapes=[pltpu.SemaphoreType.DMA((7,))],
        name="copies",
    )(place, self_block)


def whole_body(self_block, ordering, interp, near_band, pair_mask):
    boxes = ordering.shape[0]
    box_axis, nbr_axis = lax.axis_size("box"), lax.axis_size("nbr")
    place = lax.axis_index("nbr")
    low_side = place < nbr_axis // 2
    where = place.reshape(1)
    first, *later = copies(where, self_block)
    blocks_0 = exchanged(first)
    edge_start = jnp.where(low_side, 0, boxes - REACH)
    edge = lax.dynamic_slice_in_dim(near_band, edge_start, REACH, 0)
    edge_mask = jnp.where(low_side, pair_mask[:REACH], pair_mask[boxes - REACH :]).astype(F32)
    halo = lax.ppermute(
        edge * edge_mask[:, :, None, None, None],
        ("box", "nbr"),
        toward(box_axis, nbr_axis, True),
    )
    blocks_1 = []
    for k in range(3):
        turn = [(i, (i + k + 1) % nbr_axis) for i in range(nbr_axis)]
        blocks_1.append(lax.ppermute(later[k], "nbr", turn))
    wide = pltpu.VMEM((HALF, 2, PTS, PTS), BF)
    tail = pltpu.VMEM((HALF, RED, PTS), F32)
    extended = pltpu.VMEM((16, SKEL, PAIR), F32)
    all_blocks = pltpu.VMEM((4, HALF, SKEL, PTS), F32)
    some_interp = pltpu.VMEM((HALF, SKEL, RED), F32)
    kept_shape = shape(HALF, SKEL, PAIR)
    pair_shape = shape(HALF, 2, PTS, PTS, dtype=BF)
    inverse_shape = shape(boxes, ROWS, RED)
    couple_shape, own_shape = shape(boxes, 2, SKEL, PAIR), shape(boxes, SKEL, SKEL)

    def halves(x, chunk):
        return part(x, lambda p: half_of(p, chunk))

    inverse, z, s, inv, skel, side = call(
        factor_kernel, where,
        [whole(ordering), untouched(interp), untouched(blocks_0)],
        [
            halves(inverse_shape, 0), whole(pair_shape), whole(pair_shape),
            whole(shape(HALF, 8, PTS)), whole(shape(HALF, SKEL, PTS)),
            whole(shape(HALF, PTS, PAIR)),
        ],
        [all_blocks, some_interp, wide, wide, tail, pltpu.SemaphoreType.DMA((2,))],
    )
    couple, own, kept, leaving = call(
        edge_kernel, where,
        [
            smem(pair_mask), whole(near_band), whole(halo), whole(z), whole(s), whole(inv),
            whole(skel), whole(side),
        ],
        [
            halves(couple_shape, 0), halves(own_shape, 0), whole(kept_shape), whole(kept_shape),
        ],
        [extended],
    )
    came = lax.ppermute(leaving, ("box", "nbr"), toward(box_axis, nbr_axis, False))
    red_inverse, couplings, own, total = call(
        inner_kernel, where,
        [
            smem(pair_mask), whole(ordering), untouched(interp), whole(near_band),
            untouched(self_block), *[untouched(b) for b in blocks_1], whole(kept),
            untouched(inverse), untouched(couple), untouched(own),
        ],
        [
            halves(inverse_shape, 1), halves(couple_shape, 1), halves(own_shape, 1),
            whole(kept_shape),
        ],
        [
            all_blocks, some_interp, wide, wide, wide, wide, tail, extended,
            pltpu.SemaphoreType.DMA((5,)),
        ],
        {10: 0, 11: 1, 12: 2},
    )
    lane_left = lax.broadcasted_iota(jnp.int32, (1, 1, PAIR), 2) < SKEL
    total = total + jnp.where(lane_left == low_side, came, 0.0)
    flat = total.reshape(HALF * SKEL, PAIR)
    gathered = exchanged(jnp.concatenate([flat] * 4)).sum(axis=0).reshape(HALF, SKEL, PAIR)
    update = jnp.concatenate([gathered[:, :, :SKEL], gathered[:, :, SKEL:]], axis=0)
    return own - update, red_inverse, couplings


def solution(mesh):
    placed = (
        P("box", "nbr", None),
        P("box", None),
        P("box", None, None),
        P("box", "nbr", None, None, None),
        P("box", "nbr"),
    )
    return jax.shard_map(
        whole_body,
        mesh=mesh,
        in_specs=placed,
        out_specs=(P("box", None, None), P("box", "nbr", None), P("box", "nbr", None, None)),
        check_vma=False,
    )
```

```python
import jax
import jax.numpy as jnp
from jax import lax
from jax.experimental import pallas as pl
from jax.experimental.pallas import tpu as pltpu
from jax.sharding import PartitionSpec as P

SKEL = 64
RED = 192
PTS = 256
REACH = 4
HALF = 4
PAIR = 128
ROWS = 48
BF = jnp.bfloat16
F32 = jnp.float32
LIMIT = 28 * 1024 * 1024


def split(x):
    high = x.astype(BF)
    return high, (x - high.astype(F32)).astype(BF)


def dot(a, b):
    return jnp.dot(a, b, preferred_element_type=F32)


def dot3(a, b):
    return dot(a[0], b[0]) + dot(a[1], b[0]) + dot(a[0], b[1])


def eye(rows, columns):
    i = lax.broadcasted_iota(jnp.int32, (rows, columns), 0)
    j = lax.broadcasted_iota(jnp.int32, (rows, columns), 1)
    return (i == j).astype(F32)


def slot_offset(place, slot):
    j = place * 2 + slot
    return jnp.where(j < REACH, j - REACH, j - REACH + 1)


def half_of(place, chunk):
    return jnp.where(place < 2, 1 - chunk, chunk)


def choose(boxes, order_ref, interp, z_ref, zt_ref):
    unknown = lax.broadcasted_iota(jnp.int32, (PTS, PTS), 0)
    column = lax.broadcasted_iota(jnp.int32, (PTS, PTS), 1)
    lane = lax.broadcasted_iota(jnp.int32, (1, PAIR), 1)
    one, nothing = eye(SKEL, SKEL).astype(BF), jnp.zeros((SKEL, SKEL), BF)
    for k, box in enumerate(boxes):
        order = order_ref[pl.ds(box, 1), :]
        red = jnp.logical_and(unknown == pltpu.roll(order, RED, 1), column < RED).astype(F32)
        twice = jnp.where(lane < SKEL, order[:, :PAIR], pltpu.roll(order, SKEL, 1)[:, :PAIR])
        skel = (unknown[:, :PAIR] == twice).astype(F32).astype(BF)
        high, low = split(-interp[k])
        both = jnp.concatenate(
            [jnp.concatenate([high, one], axis=1), jnp.concatenate([low, nothing], axis=1)], axis=0
        )
        z = red + dot(skel, both)
        z_ref[k, 0], z_ref[k, 1] = split(z)
        zt_ref[k, 0], zt_ref[k, 1] = split(z.T)


def meet(boxes, place, mask_ref, near_ref, halo_ref, z_ref):
    g, nt = [], []
    for k, box in enumerate(boxes):
        rows = []
        for slot in range(2):
            source = box - slot_offset(place, slot)
            inside = jnp.logical_and(source >= 0, source < 2 * HALF)
            local = jnp.clip(source, 0, 2 * HALF - 1)
            weight = jnp.where(inside, mask_ref[local, slot], 0).astype(F32)
            row = near_ref[local, slot] * weight
            if halo_ref is not None:
                remote = jnp.where(source >= 2 * HALF, source - 2 * HALF, source + HALF)
                remote = jnp.clip(remote, 0, HALF - 1)
                row = row + halo_ref[remote, slot] * jnp.where(inside, 0, 1).astype(F32)
            rows.append(row)
        stacked = jnp.concatenate([rows[0][0], rows[1][0], rows[0][1], rows[1][1]], axis=0)
        done = dot3(split(stacked), (z_ref[k, 0], z_ref[k, 1]))
        g.append(done[:PAIR])
        nt.append(done[PAIR:].T)
    return g, nt


def factor(place, blocks_ref, z_ref, zt_ref, even, odd, tail, inverse_ref):
    each = range(HALF)
    diagonal = eye(PTS, PTS)
    red_diag = diagonal[:RED]
    column = lax.broadcasted_iota(jnp.int32, (1, PTS), 1)
    moved, diag_row, block, inv = [], [], [], []
    for k in each:
        full = blocks_ref[:, k].reshape(PTS, PTS)
        diag_row.append(jnp.sum(full * diagonal, axis=0, keepdims=True))
        moved.append(split(dot3(split(full), (z_ref[k, 0], z_ref[k, 1]))))
    for k in each:
        block.append(dot3((zt_ref[k, 0], zt_ref[k, 1]), moved[k]))
    for k in each:
        chosen = zt_ref[k, 0].astype(F32)
        order_col = jnp.sum(jnp.where(chosen == 1.0, diag_row[k], 0.0), axis=1, keepdims=True)
        scale = jnp.sum(diagonal * order_col, axis=0, keepdims=True)
        inv.append(jnp.where(column < RED, 1.0 / jnp.where(column < RED, scale, 1.0), 0.0))
    nothing = jnp.zeros((SKEL, PTS), BF)
    e1, e1s, e2, s4 = [], [], [], []
    for k in each:
        for ref in (even, odd):
            ref[k, 0, RED:], ref[k, 1, RED:] = nothing, nothing
        e1.append(jnp.where(column < RED, red_diag - block[k][:RED] * inv[k], 0.0))
        e1s.append(split(e1[k]))
        even[k, 0, :RED], even[k, 1, :RED] = e1s[k]
    for k in each:
        e2.append(dot3(e1s[k], (even[k, 0], even[k, 1])))
        odd[k, 0, :RED], odd[k, 1, :RED] = split(e2[k])
    for k in each:
        e2s = (odd[k, 0, :RED], odd[k, 1, :RED])
        e4 = dot3(e2s, (odd[k, 0], odd[k, 1]))
        s4.append(red_diag + e1[k] + e2[k] + dot3(e1s[k], (odd[k, 0], odd[k, 1])))
        even[k, 0, :RED], even[k, 1, :RED] = split(e4)
    for k in each:
        s8 = s4[k] + dot3(split(s4[k]), (even[k, 0], even[k, 1]))
        odd[k, 0, :RED], odd[k, 1, :RED] = split(s8)
        tail[k] = s8
    i = lax.broadcasted_iota(jnp.int32, (ROWS, PTS), 0) + place * ROWS
    j = lax.broadcasted_iota(jnp.int32, (ROWS, PTS), 1)
    start = pl.multiple_of(place * ROWS, 8)
    for k in each:
        inv_col = jnp.sum(jnp.where(i == j, inv[k], 0.0), axis=1, keepdims=True)
        inverse_ref[k] = (tail[k, pl.ds(start, ROWS), :] * inv_col)[:, :RED]
    skel = [block[k][RED:] for k in each]
    side = [block[k][:, PAIR:] for k in each]
    return inv, skel, side


def finish(boxes, place, inv, skel, side, g, nt, s_ref, couple_ref, own_ref, extended):
    each = range(HALF)
    lane = lax.broadcasted_iota(jnp.int32, (SKEL, PAIR), 1)
    left = lane < SKEL
    carried, last = [], []
    for k in each:
        mine = jnp.concatenate([skel[k], g[k]], axis=0) * inv[k]
        carried.append(dot3(split(mine), (s_ref[k, 0], s_ref[k, 1])))
    for k in each:
        right = split(jnp.concatenate([nt[k], side[k]], axis=1))
        last.append(dot3(split(carried[k]), right))
    for k in each:
        end = last[k]
        own_ref[k] = (skel[k][:, PAIR:] - end[:SKEL, PAIR:])[:, SKEL:]
        forward = nt[k][RED:] - end[:SKEL, :PAIR]
        backward = (g[k][:, PAIR:] - end[SKEL:, PAIR:]).T[SKEL:]
        couple_ref[k, 0] = jnp.where(left, forward, pltpu.roll(backward, SKEL, 1))
        couple_ref[k, 1] = jnp.where(left, pltpu.roll(forward, SKEL, 1), backward)
    for k, box in enumerate(boxes):
        first = box - slot_offset(place, 0) + REACH
        second = box - slot_offset(place, 1) + REACH
        extended[first] += jnp.where(left, last[k][SKEL:PAIR, :PAIR], 0.0)
        extended[second] += jnp.where(left, 0.0, last[k][PAIR:, :PAIR])
    return left


def doubled(x):
    return x + pltpu.roll(x, SKEL, 1)


def packed(extended, left):
    return [
        jnp.where(left, doubled(extended[REACH + k]), doubled(extended[REACH + HALF + k]))
        for k in range(HALF)
    ]


def boxes_of(place, chunk):
    base = half_of(place, chunk) * HALF
    return [base + k for k in range(HALF)]


def started(copies):
    for copy in copies:
        copy.start()
    return copies


def ended(copies):
    for copy in copies:
        copy.wait()


def half_rows(ref, place, chunk):
    return ref.at[pl.ds(half_of(place, chunk) * HALF, HALF)]


def factor_kernel(
    place_ref, order_ref, interp_ref, first_ref,
    inverse_ref, z_ref, s_ref, inv_ref, skel_ref, side_ref,
    blocks_ref, interp, zt_ref, even, tail, sem,
):
    place = place_ref[0]
    needs = started([
        pltpu.make_async_copy(half_rows(interp_ref, place, 0), interp, sem.at[0]),
        pltpu.make_async_copy(first_ref, blocks_ref, sem.at[1]),
    ])
    ended(needs[:1])
    choose(boxes_of(place, 0), order_ref, interp, z_ref, zt_ref)
    ended(needs[1:])
    inv, skel, side = factor(place, blocks_ref, z_ref, zt_ref, even, s_ref, tail, inverse_ref)
    for k in range(HALF):
        inv_ref[k] = jnp.broadcast_to(inv[k], (8, PTS))
        skel_ref[k], side_ref[k] = skel[k], side[k]


def edge_kernel(
    place_ref, mask_ref, near_ref, halo_ref, z_ref, s_ref, inv_ref, skel_ref, side_ref,
    couple_ref, own_ref, kept_ref, leaving_ref, extended,
):
    place = place_ref[0]
    boxes = boxes_of(place, 0)
    extended[...] = jnp.zeros_like(extended)
    g, nt = meet(boxes, place, mask_ref, near_ref, halo_ref, z_ref)
    inv = [inv_ref[k, :1] for k in range(HALF)]
    skel = [skel_ref[k] for k in range(HALF)]
    side = [side_ref[k] for k in range(HALF)]
    left = finish(boxes, place, inv, skel, side, g, nt, s_ref, couple_ref, own_ref, extended)
    for k, value in enumerate(packed(extended, left)):
        kept_ref[k] = value
    beyond = jnp.where(place < 2, REACH + 2 * HALF, 0)
    for k in range(HALF):
        leaving_ref[k] = doubled(extended[beyond + k])


def inner_kernel(
    place_ref, mask_ref, order_ref, interp_ref, near_ref, block_ref, came_1, came_2, came_3,
    kept_in, inverse_in, couple_in, own_in,
    inverse_ref, couple_ref, own_ref, total_ref,
    blocks_ref, interp, z_ref, zt_ref, even, odd, tail, extended, sem,
):
    place = place_ref[0]
    boxes = boxes_of(place, 1)
    text = started([pltpu.make_async_copy(half_rows(interp_ref, place, 1), interp, sem.at[4])])
    parts = started([
        pltpu.make_async_copy(source, blocks_ref.at[lax.rem(place + 4 - k, 4)], sem.at[k])
        for k, source in enumerate([half_rows(block_ref, place, 1), came_1, came_2, came_3])
    ])
    extended[...] = jnp.zeros_like(extended)
    ended(text)
    choose(boxes, order_ref, interp, z_ref, zt_ref)
    ended(parts)
    inv, skel, side = factor(place, blocks_ref, z_ref, zt_ref, even, odd, tail, inverse_ref)
    g, nt = meet(boxes, place, mask_ref, near_ref, None, z_ref)
    left = finish(boxes, place, inv, skel, side, g, nt, odd, couple_ref, own_ref, extended)
    for k, value in enumerate(packed(extended, left)):
        total_ref[k] = value + kept_in[k]


def call(kernel, place, args, outs, scratch, aliases=None):
    def spec(x):
        if isinstance(x, pl.BlockSpec):
            return x
        shape = x.shape
        return pl.BlockSpec(shape, lambda i, p: (0,) * len(shape))

    return pl.pallas_call(
        kernel,
        grid_spec=pltpu.PrefetchScalarGridSpec(
            num_scalar_prefetch=1,
            grid=(1,),
            in_specs=[spec(s) for _, s in args],
            out_specs=[spec(s) for _, s in outs],
            scratch_shapes=scratch,
        ),
        out_shape=[o for o, _ in outs],
        input_output_aliases=aliases or {},
        compiler_params=pltpu.CompilerParams(vmem_limit_bytes=LIMIT),
    )(place, *[a for a, _ in args])


def whole(x):
    return (x, x)


def part(x, index):
    shape = (HALF, *x.shape[1:])
    if callable(index):
        return (x, pl.BlockSpec(shape, lambda i, p: (index(p[0]),) + (0,) * (len(shape) - 1)))
    return (x, pl.BlockSpec(shape, lambda i, p: (index,) + (0,) * (len(shape) - 1)))


def smem(x):
    return (x, pl.BlockSpec(memory_space=pltpu.SMEM))


def untouched(x):
    return (x, pl.BlockSpec(memory_space=pl.ANY))


def shape(*s, dtype=F32):
    return jax.ShapeDtypeStruct(s, dtype)


def toward(box_count, nbr_count, receive):
    pairs = []
    for box in range(box_count):
        for place in range(nbr_count):
            step = 1 if (place < nbr_count // 2) == receive else -1
            other = (box + step) % box_count
            pairs.append((other * nbr_count + place, box * nbr_count + place))
    return pairs


def exchanged(x):
    return lax.all_to_all(x, "nbr", 0, 0, tiled=True).reshape(4, -1, *x.shape[1:])


def copies_kernel(place_ref, block_ref, first_ref, *rest):
    later, sem = rest[:3], rest[3]
    place = place_ref[0]
    copies = []
    for target in range(4):
        half = HALF * (1 if target < 2 else 0)
        copies.append((half, first_ref.at[pl.ds(target * HALF, HALF)]))
    for k in range(3):
        target = lax.rem(place + k + 1, 4)
        copies.append((HALF * half_of(target, 1), later[k]))
    copies = [
        pltpu.make_async_copy(block_ref.at[pl.ds(half, HALF)], out, sem.at[k])
        for k, (half, out) in enumerate(copies)
    ]
    for copy in copies:
        copy.start()
    for copy in copies:
        copy.wait()


def copies(place, self_block):
    anywhere = pl.BlockSpec(memory_space=pl.ANY)
    rest = self_block.shape[1:]
    return pl.pallas_call(
        copies_kernel,
        in_specs=[
            pl.BlockSpec(memory_space=pltpu.SMEM), pl.BlockSpec(memory_space=pltpu.VMEM),
        ],
        out_specs=[anywhere] * 4,
        out_shape=[shape(4 * HALF, *rest)] + [shape(HALF, *rest)] * 3,
        scratch_shapes=[pltpu.SemaphoreType.DMA((7,))],
        name="copies",
    )(place, self_block)


def whole_body(self_block, ordering, interp, near_band, pair_mask):
    boxes = ordering.shape[0]
    box_axis, nbr_axis = lax.axis_size("box"), lax.axis_size("nbr")
    place = lax.axis_index("nbr")
    low_side = place < nbr_axis // 2
    where = place.reshape(1)
    first, *later = copies(where, self_block)
    blocks_0 = exchanged(first)
    edge_start = jnp.where(low_side, 0, boxes - REACH)
    edge = lax.dynamic_slice_in_dim(near_band, edge_start, REACH, 0)
    edge_mask = jnp.where(low_side, pair_mask[:REACH], pair_mask[boxes - REACH :]).astype(F32)
    halo = lax.ppermute(
        edge * edge_mask[:, :, None, None, None],
        ("box", "nbr"),
        toward(box_axis, nbr_axis, True),
    )
    blocks_1 = []
    for k in range(3):
        turn = [(i, (i + k + 1) % nbr_axis) for i in range(nbr_axis)]
        blocks_1.append(lax.ppermute(later[k], "nbr", turn))
    wide = pltpu.VMEM((HALF, 2, PTS, PTS), BF)
    tail = pltpu.VMEM((HALF, RED, PTS), F32)
    extended = pltpu.VMEM((16, SKEL, PAIR), F32)
    all_blocks = pltpu.VMEM((4, HALF, SKEL, PTS), F32)
    some_interp = pltpu.VMEM((HALF, SKEL, RED), F32)
    kept_shape = shape(HALF, SKEL, PAIR)
    pair_shape = shape(HALF, 2, PTS, PTS, dtype=BF)
    inverse_shape = shape(boxes, ROWS, RED)
    couple_shape, own_shape = shape(boxes, 2, SKEL, PAIR), shape(boxes, SKEL, SKEL)

    def halves(x, chunk):
        return part(x, lambda p: half_of(p, chunk))

    inverse, z, s, inv, skel, side = call(
        factor_kernel, where,
        [whole(ordering), untouched(interp), untouched(blocks_0)],
        [
            halves(inverse_shape, 0), whole(pair_shape), whole(pair_shape),
            whole(shape(HALF, 8, PTS)), whole(shape(HALF, SKEL, PTS)),
            whole(shape(HALF, PTS, PAIR)),
        ],
        [all_blocks, some_interp, wide, wide, tail, pltpu.SemaphoreType.DMA((2,))],
    )
    couple, own, kept, leaving = call(
        edge_kernel, where,
        [
            smem(pair_mask), whole(near_band), whole(halo), whole(z), whole(s), whole(inv),
            whole(skel), whole(side),
        ],
        [
            halves(couple_shape, 0), halves(own_shape, 0), whole(kept_shape), whole(kept_shape),
        ],
        [extended],
    )
    came = lax.ppermute(leaving, ("box", "nbr"), toward(box_axis, nbr_axis, False))
    red_inverse, couplings, own, total = call(
        inner_kernel, where,
        [
            smem(pair_mask), whole(ordering), untouched(interp), whole(near_band),
            untouched(self_block), *[untouched(b) for b in blocks_1], whole(kept),
            untouched(inverse), untouched(couple), untouched(own),
        ],
        [
            halves(inverse_shape, 1), halves(couple_shape, 1), halves(own_shape, 1),
            whole(kept_shape),
        ],
        [
            all_blocks, some_interp, wide, wide, wide, wide, tail, extended,
            pltpu.SemaphoreType.DMA((5,)),
        ],
        {10: 0, 11: 1, 12: 2},
    )
    lane_left = lax.broadcasted_iota(jnp.int32, (1, 1, PAIR), 2) < SKEL
    total = total + jnp.where(lane_left == low_side, came, 0.0)
    flat = total.reshape(HALF * SKEL, PAIR)
    gathered = exchanged(jnp.concatenate([flat] * 4)).sum(axis=0).reshape(HALF, SKEL, PAIR)
    update = jnp.concatenate([gathered[:, :, :SKEL], gathered[:, :, SKEL:]], axis=0)
    return own - update, red_inverse, couplings


def solution(mesh):
    placed = (
        P("box", "nbr", None),
        P("box", None),
        P("box", None, None),
        P("box", "nbr", None, None, None),
        P("box", "nbr"),
    )
    return jax.shard_map(
        whole_body,
        mesh=mesh,
        in_specs=placed,
        out_specs=(P("box", None, None), P("box", "nbr", None), P("box", "nbr", None, None)),
        check_vma=False,
    )
```
